32 devices in a mesh: row: 4 (over z), col: 8 (over y, x, core).
Axes of the slice: x: 2, y: 2, z: 4, core: 2. Of those that a mesh axis runs over, the one named last changes fastest.
Arguments:
- points: float32 [16, 32768], P(None, ('row', 'col')), may hold values from -6 to 6
- inverse_scales: float32 [16], replicated, may hold values from 0.05 to 31.255105
- probe_signs: int32 [32768, 128], P(('row', 'col')), may hold values 0 or 1
Outputs:
- trace_terms: float32 [128], replicated
- logdet_terms: float32 [128], replicated
The draws below stay inside these ranges and needn't reach their ends.
All inputs are finite; a program needn't handle non-finite values. No bound on the sum of `probe_signs` on one device may be relied on, other than what follows from the above.
Results may differ from the reference program's by a relative error of at most 0.0014.
Values may be sent and summed in bfloat16 or wider, within the bound.
A program may use at most 128 MiB of HBM per device.

```python
import math
import jax
import jax.numpy as jnp
from jax import lax

N = 32768
DIM = 16
PROBES = 128
STEPS = 3


def cluster_table(key):
    level_key, slot_key = jax.random.split(jax.random.fold_in(key, 29))
    positions = jnp.arange(N, dtype=jnp.int32)
    level_draw = jax.random.randint(level_key, (N,), 0, 6)
    levels = jnp.minimum(level_draw, 3)
    block_sizes = [max(N // 128, 1), max(N // 32, 1), max(N // 8, 1), N]
    counts = [max(block_sizes[0] // 60, 1), max(block_sizes[1] // 60, 1), max(block_sizes[2] // 60, 1), max(N // 20, 1)]
    raw_slots = jax.random.randint(slot_key, (N,), 0, 1 << 20)
    table_rows = jnp.zeros((N,), jnp.int32)
    for level_num in range(4):
        slot_ids = raw_slots % counts[level_num]
        candidate = level_num * N + positions // block_sizes[level_num] * counts[level_num] + slot_ids
        table_rows = jnp.where(levels == level_num, candidate, table_rows)
    return table_rows.astype(jnp.int32)


def draw_points(key, part):
    table_rows = cluster_table(key)
    centre_key, jitter_key = jax.random.split(jax.random.fold_in(key, 41))
    centres = jax.random.normal(centre_key, (DIM, 4 * N), jnp.float32)
    jitter = 0.5 * jax.random.normal(jitter_key, (DIM, N), jnp.float32)
    return jnp.clip(centres[:, table_rows] + jitter, -6.0, 6.0)


def draw_inverse_scales(key, part):
    second_key = jax.random.fold_in(jax.random.fold_in(key, 17), 1)
    return jnp.exp(jax.random.uniform(second_key, (DIM,), jnp.float32, math.log(0.25), math.log(0.5)))


def touch_ends(array, stream_key, low, largest):
    longest = array.shape.index(max(array.shape))
    spots = []
    for shift in (0, 1):
        where = [jax.random.randint(jax.random.fold_in(stream_key, axis), (), 0, length) for axis, length in enumerate(array.shape)]
        where[longest] = (where[longest] + shift) % array.shape[longest]
        spots.append(tuple(where))
    return array.at[spots[0]].set(low).at[spots[1]].set(largest)


def setup_inputs(seed: int = 0) -> dict:
    key_of = jax.random.split(jax.random.key(seed), 4)
    points = draw_points(jax.random.fold_in(key_of[3], 71), 0)
    inverse_scales = draw_inverse_scales(jax.random.fold_in(key_of[3], 71), 0)
    probe_signs = touch_ends((jax.random.randint(key_of[2], (N, PROBES), 0, 2) < 1).astype(jnp.int32), jax.random.fold_in(key_of[2], 1), 0, 1)
    return {"points": points, "inverse_scales": inverse_scales, "probe_signs": probe_signs}


epsilon = 1e-06
noise_level = 1.0
jacobi_sweeps = 6

def kernel_block(left_points, right_points):
    cross_term = lax.dot_general(left_points, right_points, (((0,), (0,)), ((), ())), precision=lax.Precision.HIGHEST, preferred_element_type=jnp.float32)
    left_norms = lax.optimization_barrier(jnp.sum(left_points * left_points, axis=0))
    right_norms = lax.optimization_barrier(jnp.sum(right_points * right_points, axis=0))
    distance = jnp.maximum(left_norms[:, None] + right_norms[None, :] - 2.0 * cross_term, 0.0)
    return jnp.exp(-0.5 * distance).astype(jnp.bfloat16)

def apply_kernel(scaled, vector_half):
    total_rows = scaled.shape[1]
    block_rows = math.gcd(total_rows, 2048)
    blocked = scaled.reshape(scaled.shape[0], total_rows // block_rows, block_rows).transpose(1, 0, 2)
    products = lax.map(lambda block_points: jnp.dot(kernel_block(block_points, scaled), vector_half, preferred_element_type=jnp.float32), blocked)
    return products.reshape(total_rows, vector_half.shape[1])

def log_weight(alpha_list, beta_list):
    degree = len(alpha_list)
    width_probes = alpha_list[0].shape[0]
    zeros_row = jnp.zeros((width_probes,), jnp.float32)
    ones_row = jnp.ones((width_probes,), jnp.float32)
    matrix = []
    vectors = []
    for first_idx in range(degree):
        entries = []
        basis_row = []
        for second_idx in range(degree):
            if first_idx == second_idx:
                entries.append(alpha_list[first_idx])
                basis_row.append(ones_row)
            elif abs(first_idx - second_idx) == 1:
                entries.append(beta_list[min(first_idx, second_idx)])
                basis_row.append(zeros_row)
            else:
                entries.append(zeros_row)
                basis_row.append(zeros_row)
        matrix.append(entries)
        vectors.append(basis_row)
    for sweep_index in range(jacobi_sweeps):
        for first_idx in range(degree):
            for second_idx in range(first_idx + 1, degree):
                coupling = matrix[first_idx][second_idx]
                rotate_by = 0.5 * jnp.arctan2(2.0 * coupling, matrix[second_idx][second_idx] - matrix[first_idx][first_idx])
                cosine = jnp.cos(rotate_by)
                sine_val = jnp.sin(rotate_by)
                for row_idx in range(degree):
                    left_val = matrix[row_idx][first_idx]
                    right_val = matrix[row_idx][second_idx]
                    matrix[row_idx][first_idx] = cosine * left_val - sine_val * right_val
                    matrix[row_idx][second_idx] = sine_val * left_val + cosine * right_val
                    left_vec = vectors[row_idx][first_idx]
                    right_vec = vectors[row_idx][second_idx]
                    vectors[row_idx][first_idx] = cosine * left_vec - sine_val * right_vec
                    vectors[row_idx][second_idx] = sine_val * left_vec + cosine * right_vec
                for col_idx in range(degree):
                    upper_val = matrix[first_idx][col_idx]
                    lower_val = matrix[second_idx][col_idx]
                    matrix[first_idx][col_idx] = cosine * upper_val - sine_val * lower_val
                    matrix[second_idx][col_idx] = sine_val * upper_val + cosine * lower_val
    total = zeros_row
    for index_k in range(degree):
        total = total + vectors[0][index_k] * vectors[0][index_k] * jnp.log(matrix[index_k][index_k])
    return total

def reference(points, inverse_scales, probe_signs):
    scaled = points * inverse_scales[:, None]
    direction = 2.0 * probe_signs.astype(jnp.float32) - 1.0
    basis_prev = jnp.zeros_like(direction)
    alpha_list = []
    beta_list = []
    for lanczos_step in range(STEPS):
        squares = lax.optimization_barrier(jnp.sum(direction * direction, axis=0))
        image = apply_kernel(scaled, direction.astype(jnp.bfloat16)) + noise_level * direction
        curvature = lax.optimization_barrier(jnp.sum(direction * image, axis=0))
        beta_now = jnp.sqrt(squares + epsilon)
        alpha_now = curvature / (beta_now * beta_now)
        alpha_list.append(alpha_now)
        beta_list.append(beta_now)
        if lanczos_step + 1 < STEPS:
            basis_now = direction / beta_now
            direction = image / beta_now - alpha_now * basis_now - beta_now * basis_prev
            basis_prev = basis_now
    logdet_terms = log_weight(alpha_list, beta_list[1:])
    return (alpha_list[0], logdet_terms)
```

```python
import functools
import math

import jax
import jax.numpy as jnp
from jax import lax
from jax.experimental import pallas as pl
from jax.experimental.pallas import tpu as pltpu
from jax.sharding import PartitionSpec as P

STEPS = 3


epsilon = 1e-06
noise_level = 1.0
jacobi_sweeps = 6
MESH = pl.DeviceIdType.MESH


def flip(index, mask):
    bit = 1
    out = index
    while bit <= mask:
        if mask & bit:
            out = out + bit * (1 - 2 * ((index // bit) % 2))
        bit *= 2
    return out


def relay_bit(row_off, col_off):
    bits = [1 << k for k in range(1, 16) if col_off & (1 << k)]
    return bits[0] if row_off % 2 == 0 else bits[-1]


def plan(rows, cols):
    def key(off):
        row_off, col_off = off
        odd = col_off & 1
        depth = bin(col_off >> 1).count("1")
        when = (0.0, 8.0, 12.0, 16.0, 20.0)[depth]
        return (row_off * 10 + when + odd * (1.0 if depth != 1 else 1.5), row_off, col_off)

    order = sorted(((r, c) for r in range(rows) for c in range(cols)), key=key)
    where = {off: k for k, off in enumerate(order)}
    children = []
    for row_off, col_off in order:
        mine = []
        if col_off % 2 == 0:
            bit = 2
            while bit < cols:
                target = col_off | bit
                if not col_off & bit and relay_bit(row_off, target) == bit:
                    mine.append((0, bit, where[(row_off, target)]))
                bit *= 2
            if row_off == 0 and col_off == 0:
                for other in range(1, rows):
                    mine.append((other, 0, where[(other, 0)]))
            if cols > 1:
                mine.append((0, 1, where[(row_off, col_off + 1)]))
        children.append(mine)
    return order, children


def three_parts(x):
    high = x.astype(jnp.bfloat16).astype(jnp.float32)
    rest = x - high
    middle = rest.astype(jnp.bfloat16).astype(jnp.float32)
    low = (rest - middle).astype(jnp.bfloat16).astype(jnp.float32)
    return high, middle, low


def features(x, left):
    high, middle, low = three_parts(x)
    norm = -0.5 * jnp.sum(x * x, axis=0, keepdims=True)
    parts = three_parts(norm)
    rows = lax.broadcasted_iota(jnp.int32, x.shape, 0)
    first = 0 if left else 3
    ones_at = 3 if left else 0
    tail = jnp.where((rows >= ones_at) & (rows < ones_at + 3), 1.0, 0.0)
    for k in range(3):
        tail = jnp.where(rows == first + k, parts[k], tail)
    blank = jnp.zeros_like(x)
    if left:
        groups = [high, high, middle, middle, high, low, tail, blank]
    else:
        groups = [high, middle, high, middle, low, high, tail, blank]
    return jnp.concatenate(groups, axis=0)


def tree_sum(values):
    while len(values) > 1:
        values = [values[k] + values[k + 1] for k in range(0, len(values), 2)]
    return values[0]


def kernel(
    rows, cols, order, children,
    pts_ref, signs_ref,
    sums_ref, far_ref,
    near, stage, vecs, points, left, right, total, direction, before,
    sums_out, sums_mid, sums_col, sums_row,
    pts_recv, pts_send, vec_recv, vec_send, write_sem, read_sem,
    col_recv, col_send, row_recv, row_send,
):
    blocks = rows * cols
    half = blocks // 2
    n = pts_ref.shape[1]
    probes = signs_ref.shape[0]
    my_row, my_col = lax.axis_index("row"), lax.axis_index("col")

    def device(row_off, col_off):
        return (flip(my_row, row_off), flip(my_col, col_off))

    copies = [(k, child) for k in range(blocks) for child in children[k]]
    number = {(k, child): i for i, (k, child) in enumerate(copies)}

    def remote(buffer, own, recv, send, k, child):
        row_off, col_off, target = child
        return pltpu.make_async_remote_copy(
            src_ref=own if k == 0 else buffer.at[k],
            dst_ref=buffer.at[target],
            send_sem=send.at[number[(k, child)]],
            recv_sem=recv.at[target],
            device_id=device(row_off, col_off),
            device_id_type=MESH,
        )

    def arrived(buffer, own, recv, send, k):
        if k:
            pltpu.make_async_remote_copy(
                src_ref=buffer.at[k],
                dst_ref=buffer.at[k],
                send_sem=send.at[0],
                recv_sem=recv.at[k],
                device_id=device(0, 1),
                device_id_type=MESH,
            ).wait_recv()
        for child in children[k]:
            remote(buffer, own, recv, send, k, child).start()

    def sent(buffer, own, recv, send):
        for k, child in copies:
            remote(buffer, own, recv, send, k, child).wait_send()

    barrier = pltpu.get_barrier_semaphore()
    peers = [(0, c) for c in range(1, cols)] + [(r, 0) for r in range(1, rows)]
    for peer in peers:
        pl.semaphore_signal(barrier, inc=1, device_id=device(*peer), device_id_type=MESH)
    pl.semaphore_wait(barrier, len(peers))

    pts = (points, pts_ref, pts_recv, pts_send)
    arrived(*pts, 0)
    points[0] = pts_ref[...]
    vecs[0] = signs_ref[...]
    direction[...] = signs_ref[...].astype(jnp.float32)
    right[...] = features(pts_ref[...], False).astype(jnp.bfloat16)
    for k in range(1, blocks):
        arrived(*pts, k)

    def poll(pack, pair):
        group = max(half // 4, 1)
        for g in range(0, half, group):
            @pl.when((pair >= g) & (pair < g + group))
            def _():
                for t in range(g, min(g + group, half)):
                    @pl.when(pair == t)
                    def _():
                        for k in (2 * t, 2 * t + 1):
                            arrived(*pack, k)

    def form(k, chunk):
        left[...] = features(points[k], True).T.astype(jnp.bfloat16)
        tile = math.gcd(n, 256)

        def body(j, carry):
            part = pl.ds(pl.multiple_of(j * tile, tile), tile)
            power = jnp.dot(left[part, :], right[...], preferred_element_type=jnp.float32)
            chunk[part, :] = jnp.exp2(jnp.minimum(power, 0.0)).astype(jnp.bfloat16)
            return carry

        lax.fori_loop(0, n // tile, body, 0)

    def apply(k, chunk):
        total[...] += jnp.dot(vecs[k], chunk[...], preferred_element_type=jnp.float32)

    def write(slot, pair):
        return pltpu.make_async_copy(stage.at[slot], far_ref.at[pair], write_sem.at[slot])

    def read(slot, pair):
        return pltpu.make_async_copy(far_ref.at[pair], stage.at[slot], read_sem.at[slot])

    def column_sums(x):
        width = math.gcd(n, 128)
        folded = sum(x[:, s : s + width] for s in range(0, n, width))
        return jnp.sum(folded.T, axis=0, keepdims=True)

    def exchange(step, squares, curvature):
        sums_out[step] = jnp.concatenate(
            [squares, curvature, jnp.zeros((6, probes), jnp.float32)], axis=0
        )
        for source, target, recv, send, count, across in (
            (sums_out, sums_col, col_recv, col_send, cols, False),
            (sums_mid, sums_row, row_recv, row_send, rows, True),
        ):
            moves = [
                pltpu.make_async_remote_copy(
                    src_ref=source.at[step],
                    dst_ref=target.at[step, off],
                    send_sem=send.at[step, off],
                    recv_sem=recv.at[step, off],
                    device_id=device(off, 0) if across else device(0, off),
                    device_id_type=MESH,
                )
                for off in range(1, count)
            ]
            for move in moves:
                move.start()
            for move in moves:
                move.wait()
            result = tree_sum(
                [source[step]] + [target[step, off] for off in range(1, count)]
            )
            if not across:
                sums_mid[step] = result
        return result

    def spread(row):
        return jnp.broadcast_to(row, (probes, probes)).T

    for step in range(STEPS):
        total[...] = jnp.zeros_like(total)
        pack = (vecs, signs_ref if step == 0 else vecs.at[0], vec_recv, vec_send)
        if step == 0:
            def first(pair, carry):
                poll(pack, pair)
                slot = lax.rem(pair, 2)
                form(2 * pair, near.at[pair])
                apply(2 * pair, near.at[pair])

                @pl.when(pair >= 2)
                def _():
                    write(slot, pair - 2).wait()

                form(2 * pair + 1, stage.at[slot])
                write(slot, pair).start()
                apply(2 * pair + 1, stage.at[slot])
                return carry

            lax.fori_loop(0, half, first, 0)
            for pair in range(max(half - 2, 0), half):
                write(pair % 2, pair).wait()
        else:
            def later(pair, carry):
                poll(pack, pair)
                slot = lax.rem(pair, 2)

                @pl.when(pair + 1 < half)
                def _():
                    read(1 - slot, pair + 1).start()

                apply(2 * pair, near.at[pair])
                read(slot, pair).wait()
                apply(2 * pair + 1, stage.at[slot])
                return carry

            read(0, 0).start()
            lax.fori_loop(0, half, later, 0)
        sent(*pack)
        if step == 0:
            sent(*pts)
        now = direction[...]
        image = total[...] + noise_level * now
        result = exchange(step, column_sums(now * now), column_sums(now * image))
        squares, curvature = result[0:1], result[1:2]
        sums_ref[step] = result
        if step + 1 < STEPS:
            beta = jnp.sqrt(squares + epsilon)
            alpha = curvature / (beta * beta)
            inverse = spread(1.0 / beta)
            alpha_all, beta_all = spread(alpha), spread(beta)
            for s in range(0, n, 128):
                part = slice(s, s + 128)
                basis = direction[:, part] * inverse
                fresh = (total[:, part] + noise_level * direction[:, part]) * inverse - alpha_all * basis
                if step > 0:
                    fresh = fresh - beta_all * before[:, part]
                before[:, part] = basis
                direction[:, part] = fresh
                vecs[0, :, part] = fresh.astype(jnp.bfloat16)


def log_weight(alpha_list, beta_list):
    degree = len(alpha_list)
    width_probes = alpha_list[0].shape[0]
    zeros_row = jnp.zeros((width_probes,), jnp.float32)
    ones_row = jnp.ones((width_probes,), jnp.float32)
    matrix = []
    vectors = []
    for first_idx in range(degree):
        entries = []
        basis_row = []
        for second_idx in range(degree):
            if first_idx == second_idx:
                entries.append(alpha_list[first_idx])
                basis_row.append(ones_row)
            elif abs(first_idx - second_idx) == 1:
                entries.append(beta_list[min(first_idx, second_idx)])
                basis_row.append(zeros_row)
            else:
                entries.append(zeros_row)
                basis_row.append(zeros_row)
        matrix.append(entries)
        vectors.append(basis_row)
    for sweep_index in range(jacobi_sweeps):
        for first_idx in range(degree):
            for second_idx in range(first_idx + 1, degree):
                coupling = matrix[first_idx][second_idx]
                rotate_by = 0.5 * jnp.arctan2(
                    2.0 * coupling, matrix[second_idx][second_idx] - matrix[first_idx][first_idx]
                )
                cosine = jnp.cos(rotate_by)
                sine_val = jnp.sin(rotate_by)
                for row_idx in range(degree):
                    left_val = matrix[row_idx][first_idx]
                    right_val = matrix[row_idx][second_idx]
                    matrix[row_idx][first_idx] = cosine * left_val - sine_val * right_val
                    matrix[row_idx][second_idx] = sine_val * left_val + cosine * right_val
                    left_vec = vectors[row_idx][first_idx]
                    right_vec = vectors[row_idx][second_idx]
                    vectors[row_idx][first_idx] = cosine * left_vec - sine_val * right_vec
                    vectors[row_idx][second_idx] = sine_val * left_vec + cosine * right_vec
                for col_idx in range(degree):
                    upper_val = matrix[first_idx][col_idx]
                    lower_val = matrix[second_idx][col_idx]
                    matrix[first_idx][col_idx] = cosine * upper_val - sine_val * lower_val
                    matrix[second_idx][col_idx] = sine_val * upper_val + cosine * lower_val
    total = zeros_row
    for index_k in range(degree):
        total = total + vectors[0][index_k] * vectors[0][index_k] * jnp.log(
            matrix[index_k][index_k]
        )
    return total


def per_device(rows, cols, points, inverse_scales, probe_signs):
    dims, n = points.shape
    probes = probe_signs.shape[1]
    blocks = rows * cols
    half = blocks // 2
    order, children = plan(rows, cols)
    copies = sum(len(c) for c in children)
    scaled = points * inverse_scales[:, None] * math.sqrt(math.log2(math.e))
    signs = (2.0 * probe_signs.astype(jnp.float32) - 1.0).T.astype(jnp.bfloat16)
    dma = pltpu.SemaphoreType.DMA
    vmem = pltpu.VMEM
    sums, _ = pl.pallas_call(
        functools.partial(kernel, rows, cols, order, children),
        out_shape=(
            jax.ShapeDtypeStruct((STEPS, 8, probes), jnp.float32),
            jax.ShapeDtypeStruct((half, n, n), jnp.bfloat16),
        ),
        in_specs=[pl.BlockSpec(memory_space=pltpu.VMEM)] * 2,
        out_specs=(
            pl.BlockSpec(memory_space=pltpu.VMEM),
            pl.BlockSpec(memory_space=pl.ANY),
        ),
        scratch_shapes=[
            vmem((half, n, n), jnp.bfloat16),
            vmem((2, n, n), jnp.bfloat16),
            vmem((blocks, probes, n), jnp.bfloat16),
            vmem((blocks, dims, n), jnp.float32),
            vmem((n, 8 * dims), jnp.bfloat16),
            vmem((8 * dims, n), jnp.bfloat16),
            vmem((probes, n), jnp.float32),
            vmem((probes, n), jnp.float32),
            vmem((probes, n), jnp.float32),
            vmem((STEPS, 8, probes), jnp.float32),
            vmem((STEPS, 8, probes), jnp.float32),
            vmem((STEPS, cols, 8, probes), jnp.float32),
            vmem((STEPS, rows, 8, probes), jnp.float32),
            dma((blocks,)),
            dma((copies,)),
            dma((blocks,)),
            dma((copies,)),
            dma((2,)),
            dma((2,)),
            dma((STEPS, cols)),
            dma((STEPS, cols)),
            dma((STEPS, rows)),
            dma((STEPS, rows)),
        ],
        compiler_params=pltpu.CompilerParams(
            collective_id=0, has_side_effects=True, vmem_limit_bytes=64 * 2**20 - 65536
        ),
        name="lanczos",
    )(scaled, signs)
    beta_list = [jnp.sqrt(sums[k, 0] + epsilon) for k in range(STEPS)]
    alpha_list = [sums[k, 1] / (beta_list[k] * beta_list[k]) for k in range(STEPS)]
    return alpha_list[0], log_weight(alpha_list, beta_list[1:])


def solution(mesh):
    in_specs = (P(None, ("row", "col")), P(), P(("row", "col"), None))
    out_specs = (P(), P())
    return jax.shard_map(
        functools.partial(per_device, mesh.shape["row"], mesh.shape["col"]),
        mesh=mesh, in_specs=in_specs, out_specs=out_specs, check_vma=False,
    )
```

```python
import functools
import math

import jax
import jax.numpy as jnp
from jax import lax
from jax.experimental import pallas as pl
from jax.experimental.pallas import tpu as pltpu
from jax.sharding import PartitionSpec as P

STEPS = 3


epsilon = 1e-06
noise_level = 1.0
jacobi_sweeps = 6
MESH = pl.DeviceIdType.MESH


def flip(index, mask):
    bit = 1
    out = index
    while bit <= mask:
        if mask & bit:
            out = out + bit * (1 - 2 * ((index // bit) % 2))
        bit *= 2
    return out


def relay_bit(row_off, col_off):
    bits = [1 << k for k in range(1, 16) if col_off & (1 << k)]
    return bits[0] if row_off % 2 == 0 else bits[-1]


def plan(rows, cols):
    def key(off):
        row_off, col_off = off
        odd = col_off & 1
        depth = bin(col_off >> 1).count("1")
        when = (0.0, 8.0, 12.0, 16.0, 20.0)[depth]
        return (row_off * 10 + when + odd * (1.0 if depth != 1 else 1.5), row_off, col_off)

    order = sorted(((r, c) for r in range(rows) for c in range(cols)), key=key)
    where = {off: k for k, off in enumerate(order)}
    children = []
    for row_off, col_off in order:
        mine = []
        if col_off % 2 == 0:
            bit = 2
            while bit < cols:
                target = col_off | bit
                if not col_off & bit and relay_bit(row_off, target) == bit:
                    mine.append((0, bit, where[(row_off, target)]))
                bit *= 2
            if row_off == 0 and col_off == 0:
                for other in range(1, rows):
                    mine.append((other, 0, where[(other, 0)]))
            if cols > 1:
                mine.append((0, 1, where[(row_off, col_off + 1)]))
        children.append(mine)
    return order, children


def three_parts(x):
    high = x.astype(jnp.bfloat16).astype(jnp.float32)
    rest = x - high
    middle = rest.astype(jnp.bfloat16).astype(jnp.float32)
    low = (rest - middle).astype(jnp.bfloat16).astype(jnp.float32)
    return high, middle, low


def features(x, left):
    high, middle, low = three_parts(x)
    norm = -0.5 * jnp.sum(x * x, axis=0, keepdims=True)
    parts = three_parts(norm)
    rows = lax.broadcasted_iota(jnp.int32, x.shape, 0)
    first = 0 if left else 3
    ones_at = 3 if left else 0
    tail = jnp.where((rows >= ones_at) & (rows < ones_at + 3), 1.0, 0.0)
    for k in range(3):
        tail = jnp.where(rows == first + k, parts[k], tail)
    blank = jnp.zeros_like(x)
    if left:
        groups = [high, high, middle, middle, high, low, tail, blank]
    else:
        groups = [high, middle, high, middle, low, high, tail, blank]
    return jnp.concatenate(groups, axis=0)


def tree_sum(values):
    while len(values) > 1:
        values = [values[k] + values[k + 1] for k in range(0, len(values), 2)]
    return values[0]


def kernel(
    rows, cols, order, children,
    pts_ref, signs_ref,
    sums_ref, far_ref,
    near, stage, vecs, points, left, right, total, direction, before,
    sums_out, sums_mid, sums_col, sums_row,
    pts_recv, pts_send, vec_recv, vec_send, write_sem, read_sem,
    col_recv, col_send, row_recv, row_send,
):
    blocks = rows * cols
    half = blocks // 2
    n = pts_ref.shape[1]
    probes = signs_ref.shape[0]
    my_row, my_col = lax.axis_index("row"), lax.axis_index("col")

    def device(row_off, col_off):
        return (flip(my_row, row_off), flip(my_col, col_off))

    copies = [(k, child) for k in range(blocks) for child in children[k]]
    number = {(k, child): i for i, (k, child) in enumerate(copies)}

    def remote(buffer, own, recv, send, k, child):
        row_off, col_off, target = child
        return pltpu.make_async_remote_copy(
            src_ref=own if k == 0 else buffer.at[k],
            dst_ref=buffer.at[target],
            send_sem=send.at[number[(k, child)]],
            recv_sem=recv.at[target],
            device_id=device(row_off, col_off),
            device_id_type=MESH,
        )

    def arrived(buffer, own, recv, send, k):
        if k:
            pltpu.make_async_remote_copy(
                src_ref=buffer.at[k],
                dst_ref=buffer.at[k],
                send_sem=send.at[0],
                recv_sem=recv.at[k],
                device_id=device(0, 1),
                device_id_type=MESH,
            ).wait_recv()
        for child in children[k]:
            remote(buffer, own, recv, send, k, child).start()

    def sent(buffer, own, recv, send):
        for k, child in copies:
            remote(buffer, own, recv, send, k, child).wait_send()

    barrier = pltpu.get_barrier_semaphore()
    peers = [(0, c) for c in range(1, cols)] + [(r, 0) for r in range(1, rows)]
    for peer in peers:
        pl.semaphore_signal(barrier, inc=1, device_id=device(*peer), device_id_type=MESH)
    pl.semaphore_wait(barrier, len(peers))

    pts = (points, pts_ref, pts_recv, pts_send)
    arrived(*pts, 0)
    points[0] = pts_ref[...]
    vecs[0] = signs_ref[...]
    direction[...] = signs_ref[...].astype(jnp.float32)
    right[...] = features(pts_ref[...], False).astype(jnp.bfloat16)
    arrived(vecs, signs_ref, vec_recv, vec_send, 0)

    def poll(packs, pair, begun):
        group = max(half // 4, 1)
        for g in range(0, half, group):
            @pl.when((pair >= g) & (pair < g + group))
            def _():
                for t in range(g, min(g + group, half)):
                    @pl.when(pair == t)
                    def _():
                        for k in (2 * t, 2 * t + 1):
                            for pack in packs:
                                if k or not begun:
                                    arrived(*pack, k)

    def form(k, chunk):
        left[...] = features(points[k], True).T.astype(jnp.bfloat16)
        tile = math.gcd(n, 256)

        def body(j, carry):
            part = pl.ds(pl.multiple_of(j * tile, tile), tile)
            power = jnp.dot(left[part, :], right[...], preferred_element_type=jnp.float32)
            chunk[part, :] = jnp.exp2(jnp.minimum(power, 0.0)).astype(jnp.bfloat16)
            return carry

        lax.fori_loop(0, n // tile, body, 0)

    def apply(k, chunk):
        total[...] += jnp.dot(vecs[k], chunk[...], preferred_element_type=jnp.float32)

    def write(slot, pair):
        return pltpu.make_async_copy(stage.at[slot], far_ref.at[pair], write_sem.at[slot])

    def read(slot, pair):
        return pltpu.make_async_copy(far_ref.at[pair], stage.at[slot], read_sem.at[slot])

    def column_sums(x):
        width = math.gcd(n, 128)
        folded = sum(x[:, s : s + width] for s in range(0, n, width))
        return jnp.sum(folded.T, axis=0, keepdims=True)

    def exchange(step, squares, curvature):
        sums_out[step] = jnp.concatenate(
            [squares, curvature, jnp.zeros((6, probes), jnp.float32)], axis=0
        )
        for source, target, recv, send, count, across in (
            (sums_out, sums_col, col_recv, col_send, cols, False),
            (sums_mid, sums_row, row_recv, row_send, rows, True),
        ):
            moves = [
                pltpu.make_async_remote_copy(
                    src_ref=source.at[step],
                    dst_ref=target.at[step, off],
                    send_sem=send.at[step, off],
                    recv_sem=recv.at[step, off],
                    device_id=device(off, 0) if across else device(0, off),
                    device_id_type=MESH,
                )
                for off in range(1, count)
            ]
            for move in moves:
                move.start()
            for move in moves:
                move.wait()
            result = tree_sum(
                [source[step]] + [target[step, off] for off in range(1, count)]
            )
            if not across:
                sums_mid[step] = result
        return result

    def spread(row):
        return jnp.broadcast_to(row, (probes, probes)).T

    for step in range(STEPS):
        total[...] = jnp.zeros_like(total)
        pack = (vecs, signs_ref if step == 0 else vecs.at[0], vec_recv, vec_send)
        if step == 0:
            def first(pair, carry):
                poll((pts, pack), pair, True)
                slot = lax.rem(pair, 2)
                form(2 * pair, near.at[pair])
                apply(2 * pair, near.at[pair])

                @pl.when(pair >= 2)
                def _():
                    write(slot, pair - 2).wait()

                form(2 * pair + 1, stage.at[slot])
                write(slot, pair).start()
                apply(2 * pair + 1, stage.at[slot])
                return carry

            lax.fori_loop(0, half, first, 0)
            for pair in range(max(half - 2, 0), half):
                write(pair % 2, pair).wait()
        else:
            def later(pair, carry):
                poll((pack,), pair, False)
                slot = lax.rem(pair, 2)

                @pl.when(pair + 1 < half)
                def _():
                    read(1 - slot, pair + 1).start()

                apply(2 * pair, near.at[pair])
                read(slot, pair).wait()
                apply(2 * pair + 1, stage.at[slot])
                return carry

            read(0, 0).start()
            lax.fori_loop(0, half, later, 0)
        sent(*pack)
        if step == 0:
            sent(*pts)
        now = direction[...]
        image = total[...] + noise_level * now
        result = exchange(step, column_sums(now * now), column_sums(now * image))
        squares, curvature = result[0:1], result[1:2]
        sums_ref[step] = result
        if step + 1 < STEPS:
            beta = jnp.sqrt(squares + epsilon)
            alpha = curvature / (beta * beta)
            inverse = spread(1.0 / beta)
            alpha_all, beta_all = spread(alpha), spread(beta)
            for s in range(0, n, 128):
                part = slice(s, s + 128)
                basis = direction[:, part] * inverse
                fresh = (total[:, part] + noise_level * direction[:, part]) * inverse - alpha_all * basis
                if step > 0:
                    fresh = fresh - beta_all * before[:, part]
                before[:, part] = basis
                direction[:, part] = fresh
                vecs[0, :, part] = fresh.astype(jnp.bfloat16)


def log_weight(alpha_list, beta_list):
    degree = len(alpha_list)
    width_probes = alpha_list[0].shape[0]
    zeros_row = jnp.zeros((width_probes,), jnp.float32)
    ones_row = jnp.ones((width_probes,), jnp.float32)
    matrix = []
    vectors = []
    for first_idx in range(degree):
        entries = []
        basis_row = []
        for second_idx in range(degree):
            if first_idx == second_idx:
                entries.append(alpha_list[first_idx])
                basis_row.append(ones_row)
            elif abs(first_idx - second_idx) == 1:
                entries.append(beta_list[min(first_idx, second_idx)])
                basis_row.append(zeros_row)
            else:
                entries.append(zeros_row)
                basis_row.append(zeros_row)
        matrix.append(entries)
        vectors.append(basis_row)
    for sweep_index in range(jacobi_sweeps):
        for first_idx in range(degree):
            for second_idx in range(first_idx + 1, degree):
                coupling = matrix[first_idx][second_idx]
                rotate_by = 0.5 * jnp.arctan2(
                    2.0 * coupling, matrix[second_idx][second_idx] - matrix[first_idx][first_idx]
                )
                cosine = jnp.cos(rotate_by)
                sine_val = jnp.sin(rotate_by)
                for row_idx in range(degree):
                    left_val = matrix[row_idx][first_idx]
                    right_val = matrix[row_idx][second_idx]
                    matrix[row_idx][first_idx] = cosine * left_val - sine_val * right_val
                    matrix[row_idx][second_idx] = sine_val * left_val + cosine * right_val
                    left_vec = vectors[row_idx][first_idx]
                    right_vec = vectors[row_idx][second_idx]
                    vectors[row_idx][first_idx] = cosine * left_vec - sine_val * right_vec
                    vectors[row_idx][second_idx] = sine_val * left_vec + cosine * right_vec
                for col_idx in range(degree):
                    upper_val = matrix[first_idx][col_idx]
                    lower_val = matrix[second_idx][col_idx]
                    matrix[first_idx][col_idx] = cosine * upper_val - sine_val * lower_val
                    matrix[second_idx][col_idx] = sine_val * upper_val + cosine * lower_val
    total = zeros_row
    for index_k in range(degree):
        total = total + vectors[0][index_k] * vectors[0][index_k] * jnp.log(
            matrix[index_k][index_k]
        )
    return total


def per_device(rows, cols, points, inverse_scales, probe_signs):
    dims, n = points.shape
    probes = probe_signs.shape[1]
    blocks = rows * cols
    half = blocks // 2
    order, children = plan(rows, cols)
    copies = sum(len(c) for c in children)
    scaled = points * inverse_scales[:, None] * math.sqrt(math.log2(math.e))
    signs = (2.0 * probe_signs.astype(jnp.float32) - 1.0).T.astype(jnp.bfloat16)
    dma = pltpu.SemaphoreType.DMA
    vmem = pltpu.VMEM
    sums, _ = pl.pallas_call(
        functools.partial(kernel, rows, cols, order, children),
        out_shape=(
            jax.ShapeDtypeStruct((STEPS, 8, probes), jnp.float32),
            jax.ShapeDtypeStruct((half, n, n), jnp.bfloat16),
        ),
        in_specs=[pl.BlockSpec(memory_space=pltpu.VMEM)] * 2,
        out_specs=(
            pl.BlockSpec(memory_space=pltpu.VMEM),
            pl.BlockSpec(memory_space=pl.ANY),
        ),
        scratch_shapes=[
            vmem((half, n, n), jnp.bfloat16),
            vmem((2, n, n), jnp.bfloat16),
            vmem((blocks, probes, n), jnp.bfloat16),
            vmem((blocks, dims, n), jnp.float32),
            vmem((n, 8 * dims), jnp.bfloat16),
            vmem((8 * dims, n), jnp.bfloat16),
            vmem((probes, n), jnp.float32),
            vmem((probes, n), jnp.float32),
            vmem((probes, n), jnp.float32),
            vmem((STEPS, 8, probes), jnp.float32),
            vmem((STEPS, 8, probes), jnp.float32),
            vmem((STEPS, cols, 8, probes), jnp.float32),
            vmem((STEPS, rows, 8, probes), jnp.float32),
            dma((blocks,)),
            dma((copies,)),
            dma((blocks,)),
            dma((copies,)),
            dma((2,)),
            dma((2,)),
            dma((STEPS, cols)),
            dma((STEPS, cols)),
            dma((STEPS, rows)),
            dma((STEPS, rows)),
        ],
        compiler_params=pltpu.CompilerParams(
            collective_id=0, has_side_effects=True, vmem_limit_bytes=64 * 2**20 - 65536
        ),
        name="lanczos",
    )(scaled, signs)
    beta_list = [jnp.sqrt(sums[k, 0] + epsilon) for k in range(STEPS)]
    alpha_list = [sums[k, 1] / (beta_list[k] * beta_list[k]) for k in range(STEPS)]
    return alpha_list[0], log_weight(alpha_list, beta_list[1:])


def solution(mesh):
    in_specs = (P(None, ("row", "col")), P(), P(("row", "col"), None))
    out_specs = (P(), P())
    return jax.shard_map(
        functools.partial(per_device, mesh.shape["row"], mesh.shape["col"]),
        mesh=mesh, in_specs=in_specs, out_specs=out_specs, check_vma=False,
    )
```
